32 devices in a mesh: groups: 2 (over y), tp: 4 (over z), seq: 4 (over x, core).
Axes of the slice: x: 2, y: 2, z: 4, core: 2. Of those that a mesh axis runs over, the one named last changes fastest.
Arguments:
- kv_prefill: bfloat16 [2, 2, 8, 32768, 128], P(None, None, 'groups', ('tp', 'seq')), parts along dimension 2, may hold values from -10 to 10
- queries: bfloat16 [2, 8, 64, 128], P(None, ('groups', 'seq'), 'tp'), parts along dimension 1, may hold values from -512 to 512
- new_kv: bfloat16 [2, 2, 8, 8, 128], P(None, None, ('groups', 'seq')), parts along dimension 2, may hold values from -4.5 to 4.5
- lengths: int32 [8], P(('groups', 'seq')), parts along dimension 0, may hold values from 2048 to 4095
- page_slots: int32 [8, 256], P(('groups', 'seq')), parts along dimension 0, may hold values from 0 to 255, each once within a row
Outputs:
- decode_pool: bfloat16 [2, 2, 8, 2048, 16, 128], P(None, None, 'tp', ('groups', 'seq')), parts along dimension 3
- attention_out: bfloat16 [2, 8, 64, 128], P(None, ('groups', 'seq'), 'tp'), parts along dimension 1
The draws below stay inside these ranges and needn't reach their ends.
There are 2 independent parts, one for each index of `groups`. The reference program is written for one: setup_inputs(seed, part) draws one part's arguments, and reference() takes and returns one part's arrays. A program takes and returns all parts, laid end to end along the dimension named above; each array names one. Nothing has to cross between parts.
Inputs may be any that keep to these rules, and one draw needn't show every extreme that they name: Row b belongs to sequence b: its page j goes to slot page_slots[b, j] of the row's block of 256 slots; each row uses every slot once.
All inputs are finite; a program needn't handle non-finite values.
Results may differ from the reference program's by a relative error of at most 0.01.
Values may be sent and summed in bfloat16 or wider, within the bound.
No kernel may reach another device: no remote copies, remote signals or barrier semaphores. Data moves between devices by JAX's collectives and lax.ppermute only.
A program may use at most 64 MiB of HBM per device.

```python
import math
import jax
import jax.numpy as jnp
from jax import lax

LAYERS = 2
KVH = 8
QH = 64
DH = 128
PAGE = 16
CTX = 4096
SEQ_DEV = 1
SEQS = 4
PAGES = 256
COPIES = 8


def cache_and_query(key):
    cache_shape = (2, LAYERS, SEQS, KVH, CTX, DH)
    base_cache = jax.random.truncated_normal(jax.random.fold_in(key, 101), -4.5, 4.5, cache_shape, jnp.float32)
    base_query = jax.random.truncated_normal(jax.random.fold_in(key, 102), -4.5, 4.5, (LAYERS, SEQS, KVH, QH // KVH, DH), jnp.float32)
    cache_rows = base_cache
    query_rows = base_query
    return (cache_rows.reshape(2, LAYERS, SEQS, KVH * CTX, DH), query_rows.reshape(LAYERS, SEQS, QH, DH))


def draw_kv_prefill(key, part):
    return cache_and_query(key)[0].astype(jnp.bfloat16)


def draw_queries(key, part):
    return cache_and_query(key)[1].astype(jnp.bfloat16)


def with_ends(entries, stream_key, smallest, top_value):
    dims = entries.shape
    place = [jax.random.randint(jax.random.fold_in(stream_key, axis), (), 0, dims[axis]) for axis in range(len(dims))]
    entries = entries.at[tuple(place)].set(smallest)
    longest = dims.index(max(dims))
    place[longest] = (place[longest] + 1) % dims[longest]
    return entries.at[tuple(place)].set(top_value)


def block_scale(rng, shape, split, low, largest):
    factor_of = 1.0
    for axis_at, blocks in split:
        draws = jax.random.uniform(jax.random.fold_in(jax.random.fold_in(rng, 6), axis_at), (blocks,), jnp.float32, low / len(split), largest / len(split))
        factor_of = factor_of * jnp.repeat(jnp.exp(draws), shape[axis_at] // blocks).reshape((-1,) + (1,) * (len(shape) - 1 - axis_at))
    return factor_of


def gaussian(key, dims, scale, most, split=(), held_as=jnp.bfloat16):
    values = jax.random.normal(key, dims, jnp.float32) * scale
    if len(split) > 0:
        values = block_scale(key, dims, split, -0.22, 0.18) * values
    return jnp.clip(values, min=-most, max=most).astype(held_as)


def setup_inputs(seed: int = 0, part: int = 0) -> dict:
    seeds = jax.random.split(jax.random.key(seed), 6)
    own_keys = jax.random.split(jax.random.fold_in(seeds[5], part), 6)
    return {
        "kv_prefill": draw_kv_prefill(jax.random.fold_in(jax.random.fold_in(seeds[5], part), 71), part),
        "queries": draw_queries(jax.random.fold_in(jax.random.fold_in(seeds[5], part), 71), part),
        "new_kv": gaussian(own_keys[2], (2, LAYERS, SEQS, KVH, DH), 1.0, 4.5, ((2, 4),)),
        "lengths": with_ends(jax.random.randint(own_keys[3], (SEQS,), CTX // 2, CTX), jax.random.fold_in(own_keys[3], 1), CTX // 2, CTX - 1).astype(jnp.int32),
        "page_slots": jax.vmap(lambda own: jax.random.permutation(own, SEQ_DEV * PAGES))(jax.random.split(own_keys[4], (SEQS // SEQ_DEV))).reshape((SEQS // SEQ_DEV, SEQ_DEV * PAGES)).astype(jnp.int32),
    }


def reference(kv_prefill, queries, new_kv, lengths, page_slots):
    positions = jnp.arange(CTX, dtype=jnp.int32)
    arriving = positions[None, :] == lengths[:, None]
    cache_full = kv_prefill.reshape(2, LAYERS, SEQS, KVH, CTX, DH)
    cache_full = jnp.where(arriving[None, None, :, None, :, None], new_kv[:, :, :, :, None, :], cache_full)
    slots_block = SEQ_DEV * PAGES
    owners = jnp.arange(SEQS * PAGES, dtype=jnp.int32) // slots_block
    slot_index = owners * slots_block + page_slots.reshape(-1).astype(jnp.int32)
    paged_rows = cache_full.reshape(2, LAYERS, SEQS, KVH, PAGES, PAGE, DH).transpose(0, 1, 3, 2, 4, 5, 6)
    paged_rows = paged_rows.reshape(2, LAYERS, KVH, SEQS * PAGES, PAGE, DH)
    by_head = jnp.zeros_like(paged_rows).at[:, :, :, slot_index].set(paged_rows)
    copy_heads = jnp.arange(COPIES, dtype=jnp.int32) * KVH // COPIES
    decode_pool = jnp.take(by_head, copy_heads, axis=2)
    key_cache = cache_full[0].astype(jnp.float32)
    value_cache = cache_full[1].astype(jnp.float32)
    grouped_q = queries.astype(jnp.float32).reshape(LAYERS, SEQS, KVH, QH // KVH, DH)
    scores = jnp.einsum('lshgd,lshtd->lshgt', grouped_q, key_cache, precision=lax.Precision.HIGHEST) * (1.0 / math.sqrt(DH))
    visible = (positions[None, :] <= lengths[:, None])[None, :, None, None, :]
    masked = jnp.where(visible, scores, -1e+30)
    highest = lax.optimization_barrier(jnp.max(masked, axis=-1, keepdims=True))
    exponent = jnp.where(visible, jnp.exp(masked - highest), 0.0)
    weights = (exponent / lax.optimization_barrier(jnp.sum(exponent, axis=-1, keepdims=True))).astype(jnp.bfloat16)
    mixed_out = jnp.einsum('lshgt,lshtd->lshgd', weights.astype(jnp.float32), value_cache, precision=lax.Precision.HIGHEST)
    attention_out = mixed_out.astype(jnp.bfloat16).reshape(LAYERS, SEQS, QH, DH)
    return (decode_pool, attention_out)
```

```python
import functools
import math

import jax
import jax.numpy as jnp
from jax import lax
from jax.experimental import pallas as pl
from jax.experimental.pallas import tpu as pltpu
from jax.sharding import PartitionSpec as P

KVH = 8
PAGE = 16
CTX = 4096


def swapped(array, axis, bit):
    return lax.ppermute(array, axis, [(i, i ^ 1 << bit) for i in range(lax.axis_size(axis))])


def spread_heads(blocks, axis_dim):
    tp_ranks = lax.axis_size("tp")
    kv_rank = max(1, KVH // tp_ranks)
    fanout = tp_ranks * kv_rank // KVH
    levels = fanout.bit_length() - 1
    ordering = list(range(levels))
    my_rank = lax.axis_index("tp")
    finished = []
    for bit_index in ordering:
        partner = swapped(blocks, "tp", bit_index)
        lower_side = my_rank // (1 << bit_index) % 2 == 0
        lower_part = jnp.where(lower_side, blocks, partner)
        upper_part = jnp.where(lower_side, partner, blocks)
        higher_bits = sum((1 for earlier in finished if earlier > bit_index))
        shape_now = blocks.shape
        outer_count = 2**higher_bits
        split_shape = (
            shape_now[:axis_dim]
            + (outer_count, shape_now[axis_dim] // outer_count)
            + shape_now[axis_dim + 1 :]
        )
        paired = jnp.stack(
            (lower_part.reshape(split_shape), upper_part.reshape(split_shape)), axis=axis_dim + 1
        )
        blocks = paired.reshape(
            shape_now[:axis_dim] + (2 * shape_now[axis_dim],) + shape_now[axis_dim + 1 :]
        )
        finished.append(bit_index)
    return blocks


def repack(grouped, page_row, local_seqs):
    layers_here = grouped.shape[1]
    head_count = grouped.shape[3] // CTX
    head_dim = grouped.shape[4]
    paged_rows = grouped.reshape(
        2, layers_here, local_seqs, head_count, CTX // PAGE, PAGE, head_dim
    )
    paged_rows = paged_rows.transpose(0, 1, 3, 2, 4, 5, 6).reshape(
        2, layers_here, head_count, local_seqs * (CTX // PAGE), PAGE, head_dim
    )
    inverse = jnp.argsort(page_row)
    return jnp.take(paged_rows, inverse, axis=3)


def gathered(kv_prefill, queries, new_kv, lengths, page_slots):
    local_seqs = lengths.shape[0]
    page_row = page_slots[0]
    tp_ranks = lax.axis_size("tp")
    kv_rank = max(1, KVH // tp_ranks)
    layer_count = kv_prefill.shape[1]
    grouped = spread_heads(kv_prefill, 3)
    block_rows = kv_prefill.shape[3]
    fanout = grouped.shape[3] // block_rows
    shaped = grouped.reshape(
        2, layer_count, grouped.shape[2], fanout, 1, block_rows, grouped.shape[4]
    )
    pieces = lax.all_to_all(shaped, "seq", split_axis=2, concat_axis=4, tiled=True)
    flattened = pieces.reshape(
        2,
        pieces.shape[1],
        pieces.shape[2],
        pieces.shape[3] * pieces.shape[4] * pieces.shape[5],
        pieces.shape[6],
    )
    decode_pool = repack(flattened, page_row, local_seqs)
    first_head = lax.axis_index("tp") * KVH // tp_ranks
    fresh_rows = lax.dynamic_slice_in_dim(new_kv, first_head, kv_rank, 3)
    pages_per = CTX // PAGE
    length_now = lengths[0]
    slot_now = lax.dynamic_index_in_dim(page_row, 0 + length_now // PAGE, 0, False)
    update = fresh_rows[:, :, 0][:, :, :, None, None, :]
    decode_pool = lax.dynamic_update_slice(
        decode_pool, update, (0, 0, 0, slot_now, length_now % PAGE, 0)
    )
    slot_table = page_row.reshape(local_seqs, pages_per)
    head_dim = queries.shape[3]
    key_cache = jnp.take(decode_pool[0], slot_table, axis=2).reshape(
        layer_count, kv_rank, local_seqs, CTX, head_dim
    )
    values = jnp.take(decode_pool[1], slot_table, axis=2).reshape(
        layer_count, kv_rank, local_seqs, CTX, head_dim
    )
    grouped_q = queries.reshape(
        layer_count, local_seqs, kv_rank, queries.shape[2] // kv_rank, head_dim
    )
    scores = jnp.einsum(
        "lskgd,lkstd->lskgt", grouped_q, key_cache, preferred_element_type=jnp.float32
    ) * (1.0 / math.sqrt(head_dim))
    positions = jnp.arange(CTX, dtype=jnp.int32)
    visible = (positions[None, :] <= lengths[:, None])[None, :, None, None, :]
    masked = jnp.where(visible, scores, -1e30)
    highest = jnp.max(masked, axis=-1, keepdims=True)
    exponent = jnp.where(visible, jnp.exp(masked - highest), 0.0)
    weights = (exponent / jnp.sum(exponent, axis=-1, keepdims=True)).astype(jnp.bfloat16)
    mixed_out = jnp.einsum(
        "lskgt,lkstd->lskgd", weights, values, preferred_element_type=jnp.float32
    )
    attention_out = mixed_out.astype(jnp.bfloat16).reshape(queries.shape)
    return (decode_pool, attention_out)


def scatter_pages(slots, pieces, pool_ref, bases):
    for piece, base in zip(pieces, bases):
        kinds, pages = piece.shape[0], piece.shape[1]

        def move(j, carry):
            slot = slots[base + j]
            for k in range(kinds):
                pool_ref[k, slot] = piece[k, j]
            return carry

        lax.fori_loop(0, pages, move, 0, unroll=16)


def patch(slots, length, pool_ref, fresh):
    slot = slots[length // PAGE]
    for k in range(fresh.shape[0]):
        page = pool_ref[k, slot]
        row = lax.broadcasted_iota(jnp.int32, page.shape, 0)
        token = jnp.broadcast_to(fresh[k].astype(jnp.float32), page.shape)
        page = jnp.where(row == length % PAGE, token, page.astype(jnp.float32))
        pool_ref[k, slot] = page.astype(pool_ref.dtype)


def probabilities(q, keys, bases, length, fresh_key):
    scale = 1.0 / math.sqrt(q.shape[-1])
    new_score = jnp.sum(
        q.astype(jnp.float32) * fresh_key.astype(jnp.float32), axis=-1, keepdims=True
    ) * scale
    scores = []
    highest = new_score
    for key, base in zip(keys, bases):
        part = lax.dot_general(
            q, key, (((1,), (1,)), ((), ())), preferred_element_type=jnp.float32
        ) * scale
        position = base * PAGE + lax.broadcasted_iota(jnp.int32, part.shape, 1)
        part = jnp.where(position < length, part, -1e30)
        scores.append(part)
        highest = jnp.maximum(highest, jnp.max(part, axis=-1, keepdims=True))
    grown = [jnp.exp(part - highest) for part in scores]
    new_grown = jnp.exp(new_score - highest)
    total = new_grown
    for part in grown:
        total = total + jnp.sum(part, axis=-1, keepdims=True)
    inverse = 1.0 / total
    probs = [(part * inverse).astype(jnp.bfloat16) for part in grown]
    return probs, (new_grown * inverse).astype(jnp.bfloat16).astype(jnp.float32)


def mixed(probs, new_prob, values, fresh_value):
    out = new_prob * fresh_value.astype(jnp.float32)
    for prob, value in zip(probs, values):
        out = out + lax.dot_general(
            prob, value, (((1,), (0,)), ((), ())), preferred_element_type=jnp.float32
        )
    return out


def rows_of(piece):
    return piece.reshape(piece.shape[0] * piece.shape[1], piece.shape[2])


def head_rows(out, head, kept, heads):
    row = lax.broadcasted_iota(jnp.int32, out.shape, 0)
    mine = row // (out.shape[0] // heads) == head
    return jnp.where(mine, out, kept)


def own_kernel(parts, heads, slots, meta, own, *refs):
    others = refs[: parts - 1]
    q_ref, fresh_ref, pool_ref, out_ref = refs[parts - 1 :]
    length, head, rank_part = meta[0], meta[1], meta[2]
    pages = own.shape[3]
    bases = [(rank_part ^ e) * pages for e in range(parts)]
    pieces = [own.at[:, 0, 0]] + [other.at[:, 0] for other in others]
    pool = pool_ref.at[:, 0, 0]
    scatter_pages(slots, pieces, pool, bases)
    fresh = fresh_ref[:, 0, 0]
    patch(slots, length, pool, fresh)
    q = q_ref[0, 0]
    probs, new_prob = probabilities(
        q, [rows_of(piece[0]) for piece in pieces], bases, length, fresh[0]
    )
    out = mixed(probs, new_prob, [rows_of(piece[1]) for piece in pieces], fresh[1])
    out_ref[0, 0] = head_rows(out, head, jnp.zeros_like(out), heads).astype(out_ref.dtype)


def far_key_kernel(parts, slots, meta, *refs):
    pieces = refs[:parts]
    q_ref, fresh_ref, _, pool_ref, prob_ref, new_ref = refs[parts:]
    length, _, rank_part = meta[0], meta[1], meta[2]
    pages = pieces[0].shape[1]
    bases = [(rank_part ^ e) * pages for e in range(parts)]
    pool = pool_ref.at[:, 0, 0]
    scatter_pages(slots, pieces, pool, bases)
    fresh = fresh_ref[:, 0, 0]
    patch(slots, length, pool, fresh)
    probs, new_prob = probabilities(
        q_ref[0, 0], [rows_of(piece[0]) for piece in pieces], bases, length, fresh[0]
    )
    for e, prob in enumerate(probs):
        prob_ref[e] = prob
    new_ref[...] = jnp.broadcast_to(new_prob, new_ref.shape)


def far_value_kernel(parts, heads, slots, meta, *refs):
    pieces = refs[:parts]
    prob_ref, new_ref, fresh_ref, kept_ref, _, pool_ref, out_ref = refs[parts:]
    length, head, rank_part = meta[0], meta[1], meta[2]
    pages = pieces[0].shape[1]
    bases = [(rank_part ^ e) * pages for e in range(parts)]
    pool = pool_ref.at[:, 0, 0]
    scatter_pages(slots, pieces, pool, bases)
    fresh = fresh_ref[:, 0, 0]
    patch(slots, length, pool, fresh)
    out = mixed(
        [prob_ref[e] for e in range(parts)],
        new_ref[...],
        [rows_of(piece[0]) for piece in pieces],
        fresh[0],
    )
    kept = kept_ref[0, 0].astype(jnp.float32)
    out_ref[0, 0] = head_rows(out, head, kept, heads).astype(out_ref.dtype)


def streamed(kv_prefill, queries, new_kv, lengths, page_slots):
    ranks = lax.axis_size("seq")
    me = lax.axis_index("seq")
    kinds, layers, seqs, block_rows, dim = kv_prefill.shape
    parts = CTX // block_rows
    heads = ranks // parts
    pages = block_rows // PAGE
    slot_count = page_slots.shape[1]
    q_rows = queries.shape[2]
    slots = page_slots[0]
    my_head, my_part = me // parts, me % parts
    first_head = lax.axis_index("tp") * heads
    fresh = lax.dynamic_slice_in_dim(new_kv, first_head, heads, 3)
    fresh = fresh.reshape(kinds, layers, heads, 1, dim)
    paged = kv_prefill.reshape(kinds, layers, seqs, pages, PAGE, dim)

    def send(distance, kind, layer):
        pairs = [(i, i ^ distance) for i in range(ranks)]
        starts = (kind[0], layer[0], me ^ distance, 0, 0, 0)
        sizes = (kind[1], layer[1], 1, pages, PAGE, dim)
        piece = lax.dynamic_slice(paged, starts, sizes)
        return lax.ppermute(piece.reshape(sizes[:2] + sizes[3:]), "seq", pairs)

    near = [send(e, (0, kinds), (0, layers)) for e in range(1, parts)]
    far = {}
    for kind in range(kinds):
        for layer in range(layers):
            for group in range(1, heads):
                far[kind, layer, group] = [
                    send(group * parts + e, (kind, 1), (layer, 1)).reshape(1, pages, PAGE, dim)
                    for e in range(parts)
                ]

    pool_shape = jax.ShapeDtypeStruct((kinds, layers, heads, slot_count, PAGE, dim), kv_prefill.dtype)
    out_shape = jax.ShapeDtypeStruct(queries.shape, queries.dtype)
    meta = jnp.stack([lengths[0], my_head, my_part, me]).astype(jnp.int32)
    pool, out = pl.pallas_call(
        functools.partial(own_kernel, parts, heads),
        grid_spec=pltpu.PrefetchScalarGridSpec(
            num_scalar_prefetch=2,
            grid=(layers,),
            in_specs=[
                pl.BlockSpec((kinds, 1, 1, pages, PAGE, dim), lambda l, s, m: (0, l, m[3], 0, 0, 0))
            ]
            + [
                pl.BlockSpec((kinds, 1, pages, PAGE, dim), lambda l, s, m: (0, l, 0, 0, 0))
                for _ in near
            ]
            + [
                pl.BlockSpec((1, 1, q_rows, dim), lambda l, s, m: (l, 0, 0, 0)),
                pl.BlockSpec((kinds, 1, 1, 1, dim), lambda l, s, m: (0, l, m[1], 0, 0)),
            ],
            out_specs=[
                pl.BlockSpec(
                    (kinds, 1, 1, slot_count, PAGE, dim), lambda l, s, m: (0, l, m[1], 0, 0, 0)
                ),
                pl.BlockSpec((1, 1, q_rows, dim), lambda l, s, m: (l, 0, 0, 0)),
            ],
        ),
        out_shape=(pool_shape, out_shape),
        name="own_head",
    )(slots, meta, paged, *near, queries, fresh)

    piece_spec = pl.BlockSpec((1, pages, PAGE, dim), lambda i, s, m: (0, 0, 0, 0))
    hbm_spec = pl.BlockSpec(memory_space=pl.ANY)
    weights = {}
    for kind in range(kinds):
        for layer in range(layers):
            for group in range(1, heads):
                meta = jnp.stack([lengths[0], my_head ^ group, my_part, me]).astype(jnp.int32)
                pieces = far[kind, layer, group]
                fresh_spec = pl.BlockSpec(
                    (1, 1, 1, 1, dim), lambda i, s, m, k=kind, l=layer: (k, l, m[1], 0, 0)
                )
                pool_spec = pl.BlockSpec(
                    (1, 1, 1, slot_count, PAGE, dim),
                    lambda i, s, m, k=kind, l=layer: (k, l, m[1], 0, 0, 0),
                )
                row_spec = pl.BlockSpec(
                    (1, 1, q_rows, dim), lambda i, s, m, l=layer: (l, 0, 0, 0)
                )
                prob_spec = pl.BlockSpec((parts, q_rows, block_rows), lambda i, s, m: (0, 0, 0))
                new_spec = pl.BlockSpec((q_rows, dim), lambda i, s, m: (0, 0))
                if kind == 0:
                    pool, *weights[layer, group] = pl.pallas_call(
                        functools.partial(far_key_kernel, parts),
                        grid_spec=pltpu.PrefetchScalarGridSpec(
                            num_scalar_prefetch=2,
                            grid=(1,),
                            in_specs=[piece_spec] * parts + [row_spec, fresh_spec, hbm_spec],
                            out_specs=[pool_spec, prob_spec, new_spec],
                        ),
                        out_shape=(
                            pool_shape,
                            jax.ShapeDtypeStruct((parts, q_rows, block_rows), jnp.bfloat16),
                            jax.ShapeDtypeStruct((q_rows, dim), jnp.float32),
                        ),
                        input_output_aliases={parts + 4: 0},
                        name="far_keys",
                    )(slots, meta, *pieces, queries, fresh, pool)
                else:
                    pool, out = pl.pallas_call(
                        functools.partial(far_value_kernel, parts, heads),
                        grid_spec=pltpu.PrefetchScalarGridSpec(
                            num_scalar_prefetch=2,
                            grid=(1,),
                            in_specs=[piece_spec] * parts
                            + [prob_spec, new_spec, fresh_spec, row_spec, hbm_spec],
                            out_specs=[pool_spec, row_spec],
                        ),
                        out_shape=(pool_shape, out_shape),
                        input_output_aliases={parts + 5: 1, parts + 6: 0},
                        name="far_values",
                    )(slots, meta, *pieces, *weights[layer, group], fresh, out, pool)
    return pool, out


def body(kv_prefill, *rest):
    ranks = lax.axis_size("seq")
    block_rows = kv_prefill.shape[3]
    parts = CTX // block_rows
    if KVH % lax.axis_size("tp") == 0 and KVH // lax.axis_size("tp") * parts == ranks:
        return streamed(kv_prefill, *rest)
    return gathered(kv_prefill, *rest)


def solution(mesh):
    placed = (
        P(None, None, "groups", ("tp", "seq"), None),
        P(None, ("groups", "seq"), "tp", None),
        P(None, None, ("groups", "seq"), None, None),
        P(("groups", "seq")),
        P(("groups", "seq"), None),
    )
    return jax.shard_map(
        body,
        mesh=mesh,
        in_specs=placed,
        out_specs=(
            P(None, None, "tp", ("groups", "seq"), None, None),
            P(None, ("groups", "seq"), "tp", None),
        ),
        check_vma=False,
    )
```

```python
import functools
import math

import jax
import jax.numpy as jnp
from jax import lax
from jax.experimental import pallas as pl
from jax.experimental.pallas import tpu as pltpu
from jax.sharding import PartitionSpec as P


KVH = 8
PAGE = 16
CTX = 4096
TAIL = 48


def swapped(array, axis, bit):
    return lax.ppermute(array, axis, [(i, i ^ 1 << bit) for i in range(lax.axis_size(axis))])


def spread_heads(blocks, axis_dim):
    tp_ranks = lax.axis_size("tp")
    kv_rank = max(1, KVH // tp_ranks)
    fanout = tp_ranks * kv_rank // KVH
    levels = fanout.bit_length() - 1
    ordering = list(range(levels))
    my_rank = lax.axis_index("tp")
    finished = []
    for bit_index in ordering:
        partner = swapped(blocks, "tp", bit_index)
        lower_side = my_rank // (1 << bit_index) % 2 == 0
        lower_part = jnp.where(lower_side, blocks, partner)
        upper_part = jnp.where(lower_side, partner, blocks)
        higher_bits = sum((1 for earlier in finished if earlier > bit_index))
        shape_now = blocks.shape
        outer_count = 2**higher_bits
        split_shape = (
            shape_now[:axis_dim]
            + (outer_count, shape_now[axis_dim] // outer_count)
            + shape_now[axis_dim + 1 :]
        )
        paired = jnp.stack(
            (lower_part.reshape(split_shape), upper_part.reshape(split_shape)), axis=axis_dim + 1
        )
        blocks = paired.reshape(
            shape_now[:axis_dim] + (2 * shape_now[axis_dim],) + shape_now[axis_dim + 1 :]
        )
        finished.append(bit_index)
    return blocks


def repack(grouped, page_row, local_seqs):
    layers_here = grouped.shape[1]
    head_count = grouped.shape[3] // CTX
    head_dim = grouped.shape[4]
    paged_rows = grouped.reshape(
        2, layers_here, local_seqs, head_count, CTX // PAGE, PAGE, head_dim
    )
    paged_rows = paged_rows.transpose(0, 1, 3, 2, 4, 5, 6).reshape(
        2, layers_here, head_count, local_seqs * (CTX // PAGE), PAGE, head_dim
    )
    inverse = jnp.argsort(page_row)
    return jnp.take(paged_rows, inverse, axis=3)


def gathered(kv_prefill, queries, new_kv, lengths, page_slots):
    local_seqs = lengths.shape[0]
    page_row = page_slots[0]
    tp_ranks = lax.axis_size("tp")
    kv_rank = max(1, KVH // tp_ranks)
    layer_count = kv_prefill.shape[1]
    grouped = spread_heads(kv_prefill, 3)
    block_rows = kv_prefill.shape[3]
    fanout = grouped.shape[3] // block_rows
    shaped = grouped.reshape(
        2, layer_count, grouped.shape[2], fanout, 1, block_rows, grouped.shape[4]
    )
    pieces = lax.all_to_all(shaped, "seq", split_axis=2, concat_axis=4, tiled=True)
    flattened = pieces.reshape(
        2,
        pieces.shape[1],
        pieces.shape[2],
        pieces.shape[3] * pieces.shape[4] * pieces.shape[5],
        pieces.shape[6],
    )
    decode_pool = repack(flattened, page_row, local_seqs)
    first_head = lax.axis_index("tp") * KVH // tp_ranks
    fresh_rows = lax.dynamic_slice_in_dim(new_kv, first_head, kv_rank, 3)
    pages_per = CTX // PAGE
    length_now = lengths[0]
    slot_now = lax.dynamic_index_in_dim(page_row, 0 + length_now // PAGE, 0, False)
    update = fresh_rows[:, :, 0][:, :, :, None, None, :]
    decode_pool = lax.dynamic_update_slice(
        decode_pool, update, (0, 0, 0, slot_now, length_now % PAGE, 0)
    )
    slot_table = page_row.reshape(local_seqs, pages_per)
    head_dim = queries.shape[3]
    key_cache = jnp.take(decode_pool[0], slot_table, axis=2).reshape(
        layer_count, kv_rank, local_seqs, CTX, head_dim
    )
    values = jnp.take(decode_pool[1], slot_table, axis=2).reshape(
        layer_count, kv_rank, local_seqs, CTX, head_dim
    )
    grouped_q = queries.reshape(
        layer_count, local_seqs, kv_rank, queries.shape[2] // kv_rank, head_dim
    )
    scores = jnp.einsum(
        "lskgd,lkstd->lskgt", grouped_q, key_cache, preferred_element_type=jnp.float32
    ) * (1.0 / math.sqrt(head_dim))
    positions = jnp.arange(CTX, dtype=jnp.int32)
    visible = (positions[None, :] <= lengths[:, None])[None, :, None, None, :]
    masked = jnp.where(visible, scores, -1e30)
    highest = jnp.max(masked, axis=-1, keepdims=True)
    exponent = jnp.where(visible, jnp.exp(masked - highest), 0.0)
    weights = (exponent / jnp.sum(exponent, axis=-1, keepdims=True)).astype(jnp.bfloat16)
    mixed_out = jnp.einsum(
        "lskgt,lkstd->lskgd", weights, values, preferred_element_type=jnp.float32
    )
    attention_out = mixed_out.astype(jnp.bfloat16).reshape(queries.shape)
    return (decode_pool, attention_out)


def scatter_pages(slots, pieces, pool_ref, bases):
    for piece, base in zip(pieces, bases):
        kinds, pages = piece.shape[0], piece.shape[1]

        def move(j, carry):
            slot = slots[base + j]
            for k in range(kinds):
                pool_ref[k, slot] = piece[k, j]
            return carry

        lax.fori_loop(0, pages, move, 0, unroll=16)


def patch(slots, length, pool_ref, fresh):
    slot = slots[length // PAGE]
    for k in range(fresh.shape[0]):
        page = pool_ref[k, slot]
        row = lax.broadcasted_iota(jnp.int32, page.shape, 0)
        token = jnp.broadcast_to(fresh[k].astype(jnp.float32), page.shape)
        page = jnp.where(row == length % PAGE, token, page.astype(jnp.float32))
        pool_ref[k, slot] = page.astype(pool_ref.dtype)


def probabilities(q, keys, bases, length, fresh_key):
    scale = 1.0 / math.sqrt(q.shape[-1])
    new_score = jnp.sum(
        q.astype(jnp.float32) * fresh_key.astype(jnp.float32), axis=-1, keepdims=True
    ) * scale
    scores = []
    highest = new_score
    for key, base in zip(keys, bases):
        part = lax.dot_general(
            q, key, (((1,), (1,)), ((), ())), preferred_element_type=jnp.float32
        ) * scale
        position = base * PAGE + lax.broadcasted_iota(jnp.int32, part.shape, 1)
        part = jnp.where(position < length, part, -1e30)
        scores.append(part)
        highest = jnp.maximum(highest, jnp.max(part, axis=-1, keepdims=True))
    grown = [jnp.exp(part - highest) for part in scores]
    new_grown = jnp.exp(new_score - highest)
    total = new_grown
    for part in grown:
        total = total + jnp.sum(part, axis=-1, keepdims=True)
    inverse = 1.0 / total
    probs = [(part * inverse).astype(jnp.bfloat16) for part in grown]
    return probs, (new_grown * inverse).astype(jnp.bfloat16).astype(jnp.float32)


def mixed(probs, new_prob, values, fresh_value):
    out = new_prob * fresh_value.astype(jnp.float32)
    for prob, value in zip(probs, values):
        out = out + lax.dot_general(
            prob, value, (((1,), (0,)), ((), ())), preferred_element_type=jnp.float32
        )
    return out


def rows_of(piece):
    return piece.reshape(piece.shape[0] * piece.shape[1], piece.shape[2])


def head_rows(out, head, kept, heads):
    row = lax.broadcasted_iota(jnp.int32, out.shape, 0)
    mine = row // (out.shape[0] // heads) == head
    return jnp.where(mine, out, kept)


def own_kernel(parts, heads, slots, meta, own, *refs):
    others = refs[: parts - 1]
    q_ref, fresh_ref, pool_ref, out_ref = refs[parts - 1 :]
    length, head, rank_part = meta[0], meta[1], meta[2]
    pages = own.shape[3]
    bases = [(rank_part ^ e) * pages for e in range(parts)]
    pieces = [own.at[:, 0, 0]] + [other.at[:, 0] for other in others]
    pool = pool_ref.at[:, 0, 0]
    scatter_pages(slots, pieces, pool, bases)
    fresh = fresh_ref[:, 0, 0]
    patch(slots, length, pool, fresh)
    q = q_ref[0, 0]
    probs, new_prob = probabilities(
        q, [rows_of(piece[0]) for piece in pieces], bases, length, fresh[0]
    )
    out = mixed(probs, new_prob, [rows_of(piece[1]) for piece in pieces], fresh[1])
    out_ref[0, 0] = head_rows(out, head, jnp.zeros_like(out), heads).astype(out_ref.dtype)


def far_key_kernel(parts, slots, meta, *refs):
    pieces = refs[:parts]
    q_ref, fresh_ref, _, pool_ref, prob_ref, new_ref = refs[parts:]
    length, rank_part = meta[0], meta[2]
    pages = pieces[0].shape[1]
    bases = [(rank_part ^ e) * pages for e in range(parts)]
    pool = pool_ref.at[:, 0, 0]
    scatter_pages(slots, pieces, pool, bases)
    fresh = fresh_ref[:, 0, 0]
    patch(slots, length, pool, fresh)
    probs, new_prob = probabilities(
        q_ref[0, 0], [rows_of(piece[0]) for piece in pieces], bases, length, fresh[0]
    )
    for e, prob in enumerate(probs):
        prob_ref[e] = prob
    new_ref[...] = jnp.broadcast_to(new_prob, new_ref.shape)


def far_value_kernel(parts, heads, last, slots, meta, *refs):
    pieces = refs[:parts]
    prob_ref, new_ref, fresh_ref, kept_ref, _, pool_ref, out_ref = refs[parts:]
    length, head, rank_part = meta[0], meta[1], meta[2]
    pages = pieces[0].shape[1]
    bases = [(rank_part ^ e) * pages for e in range(parts)]
    pool = pool_ref.at[:, 0, 0]
    scatter_pages(slots, pieces, pool, bases)
    fresh = fresh_ref[:, 0, 0]
    patch(slots, length, pool, fresh)
    values = [rows_of(piece[0]) for piece in pieces]
    out = mixed(
        [prob_ref[e, :, : values[e].shape[0]] for e in range(parts)],
        new_ref[...],
        values,
        fresh[0],
    )
    kept = kept_ref[0, 0].astype(jnp.float32)
    out = head_rows(out, head, kept, heads)
    if last:
        out_ref[...] = out
    else:
        out_ref[0, 0] = out.astype(out_ref.dtype)


def tail_kernel(
    parts, heads, layer, slots, meta, piece, prob, partial, fresh, _pool, _out, pool, out,
    values, probs, sums, token, page_store, row_store, sems, load_sems,
):
    length, head, rank_part = meta[0], meta[1], meta[2]
    kind = pool.shape[0] - 1
    pages = piece.shape[1]
    dim = piece.shape[3]
    whole = prob.shape[2] // PAGE
    base = (rank_part ^ (parts - 1)) * whole + whole - pages
    loads = [
        pltpu.make_async_copy(piece.at[0], values, load_sems.at[0]),
        pltpu.make_async_copy(
            prob.at[parts - 1, :, pl.ds((whole - pages) * PAGE, pages * PAGE)],
            probs,
            load_sems.at[1],
        ),
        pltpu.make_async_copy(partial, sums, load_sems.at[2]),
        pltpu.make_async_copy(fresh.at[kind, layer, head], token, load_sems.at[3]),
    ]
    for load in loads:
        load.start()
    special = length // PAGE - base
    for j in range(pages):

        @pl.when(special != j)
        def _():
            pltpu.make_async_copy(
                piece.at[0, j], pool.at[kind, layer, head, slots[base + j]], sems.at[0]
            ).start()

    for load in loads:
        load.wait()
    inside = jnp.logical_and(special >= 0, special < pages)

    @pl.when(inside)
    def _():
        page = values[jnp.clip(special, 0, pages - 1)]
        row = lax.broadcasted_iota(jnp.int32, page.shape, 0)
        fresh_row = jnp.broadcast_to(token[...].astype(jnp.float32), page.shape)
        page = jnp.where(row == length % PAGE, fresh_row, page.astype(jnp.float32))
        page_store[...] = page.astype(page_store.dtype)
        pltpu.make_async_copy(
            page_store, pool.at[kind, layer, head, slots[length // PAGE]], sems.at[0]
        ).start()

    rest = lax.dot_general(
        probs[...], values[...].reshape(pages * PAGE, dim), (((1,), (0,)), ((), ())),
        preferred_element_type=jnp.float32,
    )
    done = sums[...]
    row_store[...] = head_rows(done + rest, head, done, heads).astype(row_store.dtype)
    store = pltpu.make_async_copy(row_store, out.at[layer, 0], sems.at[1])
    store.start()
    pltpu.make_async_copy(
        piece.at[0], pool.at[kind, layer, head, pl.ds(0, pages)], sems.at[0]
    ).wait()
    store.wait()


def streamed(kv_prefill, queries, new_kv, lengths, page_slots):
    ranks = lax.axis_size("seq")
    me = lax.axis_index("seq")
    kinds, layers, seqs, block_rows, dim = kv_prefill.shape
    parts = CTX // block_rows
    heads = ranks // parts
    pages = block_rows // PAGE
    slot_count = page_slots.shape[1]
    q_rows = queries.shape[2]
    slots = page_slots[0]
    my_head, my_part = me // parts, me % parts
    first_head = lax.axis_index("tp") * heads
    fresh = lax.dynamic_slice_in_dim(new_kv, first_head, heads, 3)
    fresh = fresh.reshape(kinds, layers, heads, 1, dim)
    paged = kv_prefill.reshape(kinds, layers, seqs, pages, PAGE, dim)

    tail_pages = pages * TAIL // 128
    token = [me]

    def send(distance, kind, layer, page=(0, pages)):
        pairs = [(i, i ^ distance) for i in range(ranks)]
        starts = (kind[0], layer[0], token[0] ^ distance, page[0], 0, 0)
        sizes = (kind[1], layer[1], 1, page[1], PAGE, dim)
        piece = lax.dynamic_slice(paged, starts, sizes)
        piece = piece.reshape(sizes[:2] + sizes[3:])
        piece, token[0] = lax.optimization_barrier((piece, token[0]))
        return lax.ppermute(piece, "seq", pairs)

    near = None
    far = {}
    final = (kinds - 1, layers - 1, heads - 1)
    for kind in range(kinds):
        for layer in range(layers):
            for group in range(1, heads):
                far[kind, layer, group] = [
                    send(
                        group * parts + e,
                        (kind, 1),
                        (layer, 1),
                        (0, pages - tail_pages)
                        if (kind, layer, group) == final and e == parts - 1
                        else (0, pages),
                    )[0]
                    for e in range(parts)
                ]
                if near is None:
                    near = [send(e, (0, kinds), (0, layers)) for e in range(1, parts)]
    tail = send(ranks - 1, (kinds - 1, 1), (layers - 1, 1), (pages - tail_pages, tail_pages))[0]

    pool_shape = jax.ShapeDtypeStruct((kinds, layers, heads, slot_count, PAGE, dim), kv_prefill.dtype)
    out_shape = jax.ShapeDtypeStruct(queries.shape, queries.dtype)
    meta = jnp.stack([lengths[0], my_head, my_part, me]).astype(jnp.int32)
    pool, out = pl.pallas_call(
        functools.partial(own_kernel, parts, heads),
        grid_spec=pltpu.PrefetchScalarGridSpec(
            num_scalar_prefetch=2,
            grid=(layers,),
            in_specs=[
                pl.BlockSpec((kinds, 1, 1, pages, PAGE, dim), lambda l, s, m: (0, l, m[3], 0, 0, 0))
            ]
            + [
                pl.BlockSpec((kinds, 1, pages, PAGE, dim), lambda l, s, m: (0, l, 0, 0, 0))
                for _ in near
            ]
            + [
                pl.BlockSpec((1, 1, q_rows, dim), lambda l, s, m: (l, 0, 0, 0)),
                pl.BlockSpec((kinds, 1, 1, 1, dim), lambda l, s, m: (0, l, m[1], 0, 0)),
            ],
            out_specs=[
                pl.BlockSpec(
                    (kinds, 1, 1, slot_count, PAGE, dim), lambda l, s, m: (0, l, m[1], 0, 0, 0)
                ),
                pl.BlockSpec((1, 1, q_rows, dim), lambda l, s, m: (l, 0, 0, 0)),
            ],
        ),
        out_shape=(pool_shape, out_shape),
        name="own_head",
    )(slots, meta, paged, *near, queries, fresh)

    def piece_specs(pieces):
        return [pl.BlockSpec(piece.shape, lambda i, s, m: (0, 0, 0, 0)) for piece in pieces]

    hbm_spec = pl.BlockSpec(memory_space=pl.ANY)
    weights = {}
    for kind in range(kinds):
        for layer in range(layers):
            for group in range(1, heads):
                meta = jnp.stack([lengths[0], my_head ^ group, my_part, me]).astype(jnp.int32)
                pieces = far[kind, layer, group]
                fresh_spec = pl.BlockSpec(
                    (1, 1, 1, 1, dim), lambda i, s, m, k=kind, l=layer: (k, l, m[1], 0, 0)
                )
                pool_spec = pl.BlockSpec(
                    (1, 1, 1, slot_count, PAGE, dim),
                    lambda i, s, m, k=kind, l=layer: (k, l, m[1], 0, 0, 0),
                )
                row_spec = pl.BlockSpec(
                    (1, 1, q_rows, dim), lambda i, s, m, l=layer: (l, 0, 0, 0)
                )
                prob_spec = pl.BlockSpec((parts, q_rows, block_rows), lambda i, s, m: (0, 0, 0))
                new_spec = pl.BlockSpec((q_rows, dim), lambda i, s, m: (0, 0))
                if kind == 0:
                    pool, *weights[layer, group] = pl.pallas_call(
                        functools.partial(far_key_kernel, parts),
                        grid_spec=pltpu.PrefetchScalarGridSpec(
                            num_scalar_prefetch=2,
                            grid=(1,),
                            in_specs=piece_specs(pieces) + [row_spec, fresh_spec, hbm_spec],
                            out_specs=[pool_spec, prob_spec, new_spec],
                        ),
                        out_shape=(
                            pool_shape,
                            jax.ShapeDtypeStruct((parts, q_rows, block_rows), jnp.bfloat16),
                            jax.ShapeDtypeStruct((q_rows, dim), jnp.float32),
                        ),
                        input_output_aliases={parts + 4: 0},
                        name="far_keys",
                    )(slots, meta, *pieces, queries, fresh, pool)
                else:
                    last = (kind, layer, group) == final
                    pool, mix = pl.pallas_call(
                        functools.partial(far_value_kernel, parts, heads, last),
                        grid_spec=pltpu.PrefetchScalarGridSpec(
                            num_scalar_prefetch=2,
                            grid=(1,),
                            in_specs=piece_specs(pieces)
                            + [prob_spec, new_spec, fresh_spec, row_spec, hbm_spec],
                            out_specs=[pool_spec, new_spec if last else row_spec],
                        ),
                        out_shape=(
                            pool_shape,
                            jax.ShapeDtypeStruct((q_rows, dim), jnp.float32) if last else out_shape,
                        ),
                        input_output_aliases={parts + 6: 0}
                        if last
                        else {parts + 5: 1, parts + 6: 0},
                        name="far_values",
                    )(slots, meta, *pieces, *weights[layer, group], fresh, out, pool)
                    if not last:
                        out = mix
    pool, out = pl.pallas_call(
        functools.partial(tail_kernel, parts, heads, layers - 1),
        grid_spec=pltpu.PrefetchScalarGridSpec(
            num_scalar_prefetch=2,
            grid=(1,),
            in_specs=[hbm_spec] * 6,
            out_specs=[hbm_spec] * 2,
            scratch_shapes=[
                pltpu.VMEM((tail_pages, PAGE, dim), jnp.bfloat16),
                pltpu.VMEM((q_rows, tail_pages * PAGE), jnp.bfloat16),
                pltpu.VMEM((q_rows, dim), jnp.float32),
                pltpu.VMEM((1, dim), jnp.bfloat16),
                pltpu.VMEM((PAGE, dim), jnp.bfloat16),
                pltpu.VMEM((q_rows, dim), jnp.bfloat16),
                pltpu.SemaphoreType.DMA((2,)),
                pltpu.SemaphoreType.DMA((4,)),
            ],
        ),
        out_shape=(pool_shape, out_shape),
        input_output_aliases={6: 0, 7: 1},
        name="tail_values",
    )(slots, meta, tail, weights[layers - 1, heads - 1][0], mix, fresh, pool, out)
    return pool, out


def body(kv_prefill, *rest):
    ranks = lax.axis_size("seq")
    block_rows = kv_prefill.shape[3]
    parts = CTX // block_rows
    if KVH % lax.axis_size("tp") == 0 and KVH // lax.axis_size("tp") * parts == ranks:
        return streamed(kv_prefill, *rest)
    return gathered(kv_prefill, *rest)


def solution(mesh):
    placed = (
        P(None, None, "groups", ("tp", "seq"), None),
        P(None, ("groups", "seq"), "tp", None),
        P(None, None, ("groups", "seq"), None, None),
        P(("groups", "seq")),
        P(("groups", "seq"), None),
    )
    return jax.shard_map(
        body,
        mesh=mesh,
        in_specs=placed,
        out_specs=(
            P(None, None, "tp", ("groups", "seq"), None, None),
            P(None, ("groups", "seq"), "tp", None),
        ),
        check_vma=False,
    )
```

```python
import functools
import math

import jax
import jax.numpy as jnp
from jax import lax
from jax.experimental import pallas as pl
from jax.experimental.pallas import tpu as pltpu
from jax.sharding import PartitionSpec as P


KVH = 8
PAGE = 16
CTX = 4096
TAIL = 32


def swapped(array, axis, bit):
    return lax.ppermute(array, axis, [(i, i ^ 1 << bit) for i in range(lax.axis_size(axis))])


def spread_heads(blocks, axis_dim):
    tp_ranks = lax.axis_size("tp")
    kv_rank = max(1, KVH // tp_ranks)
    fanout = tp_ranks * kv_rank // KVH
    levels = fanout.bit_length() - 1
    ordering = list(range(levels))
    my_rank = lax.axis_index("tp")
    finished = []
    for bit_index in ordering:
        partner = swapped(blocks, "tp", bit_index)
        lower_side = my_rank // (1 << bit_index) % 2 == 0
        lower_part = jnp.where(lower_side, blocks, partner)
        upper_part = jnp.where(lower_side, partner, blocks)
        higher_bits = sum((1 for earlier in finished if earlier > bit_index))
        shape_now = blocks.shape
        outer_count = 2**higher_bits
        split_shape = (
            shape_now[:axis_dim]
            + (outer_count, shape_now[axis_dim] // outer_count)
            + shape_now[axis_dim + 1 :]
        )
        paired = jnp.stack(
            (lower_part.reshape(split_shape), upper_part.reshape(split_shape)), axis=axis_dim + 1
        )
        blocks = paired.reshape(
            shape_now[:axis_dim] + (2 * shape_now[axis_dim],) + shape_now[axis_dim + 1 :]
        )
        finished.append(bit_index)
    return blocks


def repack(grouped, page_row, local_seqs):
    layers_here = grouped.shape[1]
    head_count = grouped.shape[3] // CTX
    head_dim = grouped.shape[4]
    paged_rows = grouped.reshape(
        2, layers_here, local_seqs, head_count, CTX // PAGE, PAGE, head_dim
    )
    paged_rows = paged_rows.transpose(0, 1, 3, 2, 4, 5, 6).reshape(
        2, layers_here, head_count, local_seqs * (CTX // PAGE), PAGE, head_dim
    )
    inverse = jnp.argsort(page_row)
    return jnp.take(paged_rows, inverse, axis=3)


def gathered(kv_prefill, queries, new_kv, lengths, page_slots):
    local_seqs = lengths.shape[0]
    page_row = page_slots[0]
    tp_ranks = lax.axis_size("tp")
    kv_rank = max(1, KVH // tp_ranks)
    layer_count = kv_prefill.shape[1]
    grouped = spread_heads(kv_prefill, 3)
    block_rows = kv_prefill.shape[3]
    fanout = grouped.shape[3] // block_rows
    shaped = grouped.reshape(
        2, layer_count, grouped.shape[2], fanout, 1, block_rows, grouped.shape[4]
    )
    pieces = lax.all_to_all(shaped, "seq", split_axis=2, concat_axis=4, tiled=True)
    flattened = pieces.reshape(
        2,
        pieces.shape[1],
        pieces.shape[2],
        pieces.shape[3] * pieces.shape[4] * pieces.shape[5],
        pieces.shape[6],
    )
    decode_pool = repack(flattened, page_row, local_seqs)
    first_head = lax.axis_index("tp") * KVH // tp_ranks
    fresh_rows = lax.dynamic_slice_in_dim(new_kv, first_head, kv_rank, 3)
    pages_per = CTX // PAGE
    length_now = lengths[0]
    slot_now = lax.dynamic_index_in_dim(page_row, 0 + length_now // PAGE, 0, False)
    update = fresh_rows[:, :, 0][:, :, :, None, None, :]
    decode_pool = lax.dynamic_update_slice(
        decode_pool, update, (0, 0, 0, slot_now, length_now % PAGE, 0)
    )
    slot_table = page_row.reshape(local_seqs, pages_per)
    head_dim = queries.shape[3]
    key_cache = jnp.take(decode_pool[0], slot_table, axis=2).reshape(
        layer_count, kv_rank, local_seqs, CTX, head_dim
    )
    values = jnp.take(decode_pool[1], slot_table, axis=2).reshape(
        layer_count, kv_rank, local_seqs, CTX, head_dim
    )
    grouped_q = queries.reshape(
        layer_count, local_seqs, kv_rank, queries.shape[2] // kv_rank, head_dim
    )
    scores = jnp.einsum(
        "lskgd,lkstd->lskgt", grouped_q, key_cache, preferred_element_type=jnp.float32
    ) * (1.0 / math.sqrt(head_dim))
    positions = jnp.arange(CTX, dtype=jnp.int32)
    visible = (positions[None, :] <= lengths[:, None])[None, :, None, None, :]
    masked = jnp.where(visible, scores, -1e30)
    highest = jnp.max(masked, axis=-1, keepdims=True)
    exponent = jnp.where(visible, jnp.exp(masked - highest), 0.0)
    weights = (exponent / jnp.sum(exponent, axis=-1, keepdims=True)).astype(jnp.bfloat16)
    mixed_out = jnp.einsum(
        "lskgt,lkstd->lskgd", weights, values, preferred_element_type=jnp.float32
    )
    attention_out = mixed_out.astype(jnp.bfloat16).reshape(queries.shape)
    return (decode_pool, attention_out)


def scatter_pages(slots, pieces, pool_ref, bases):
    for piece, base in zip(pieces, bases):
        kinds, pages = piece.shape[0], piece.shape[1]

        def move(j, carry):
            slot = slots[base + j]
            for k in range(kinds):
                pool_ref[k, slot] = piece[k, j]
            return carry

        lax.fori_loop(0, pages, move, 0, unroll=16)


def patch(slots, length, pool_ref, fresh):
    slot = slots[length // PAGE]
    for k in range(fresh.shape[0]):
        page = pool_ref[k, slot]
        row = lax.broadcasted_iota(jnp.int32, page.shape, 0)
        token = jnp.broadcast_to(fresh[k].astype(jnp.float32), page.shape)
        page = jnp.where(row == length % PAGE, token, page.astype(jnp.float32))
        pool_ref[k, slot] = page.astype(pool_ref.dtype)


def probabilities(q, keys, bases, length, fresh_key):
    scale = 1.0 / math.sqrt(q.shape[-1])
    new_score = jnp.sum(
        q.astype(jnp.float32) * fresh_key.astype(jnp.float32), axis=-1, keepdims=True
    ) * scale
    scores = []
    highest = new_score
    for key, base in zip(keys, bases):
        part = lax.dot_general(
            q, key, (((1,), (1,)), ((), ())), preferred_element_type=jnp.float32
        ) * scale
        position = base * PAGE + lax.broadcasted_iota(jnp.int32, part.shape, 1)
        part = jnp.where(position < length, part, -1e30)
        scores.append(part)
        highest = jnp.maximum(highest, jnp.max(part, axis=-1, keepdims=True))
    grown = [jnp.exp(part - highest) for part in scores]
    new_grown = jnp.exp(new_score - highest)
    total = new_grown
    for part in grown:
        total = total + jnp.sum(part, axis=-1, keepdims=True)
    inverse = 1.0 / total
    probs = [(part * inverse).astype(jnp.bfloat16) for part in grown]
    return probs, (new_grown * inverse).astype(jnp.bfloat16).astype(jnp.float32)


def mixed(probs, new_prob, values, fresh_value):
    out = new_prob * fresh_value.astype(jnp.float32)
    for prob, value in zip(probs, values):
        out = out + lax.dot_general(
            prob, value, (((1,), (0,)), ((), ())), preferred_element_type=jnp.float32
        )
    return out


def rows_of(piece):
    return piece.reshape(piece.shape[0] * piece.shape[1], piece.shape[2])


def head_rows(out, head, kept, heads):
    row = lax.broadcasted_iota(jnp.int32, out.shape, 0)
    mine = row // (out.shape[0] // heads) == head
    return jnp.where(mine, out, kept)


def own_kernel(parts, heads, slots, meta, own, *refs):
    others = refs[: parts - 1]
    q_ref, fresh_ref, pool_ref, out_ref = refs[parts - 1 :]
    length, head, rank_part = meta[0], meta[1], meta[2]
    pages = own.shape[3]
    bases = [(rank_part ^ e) * pages for e in range(parts)]
    pieces = [own.at[:, 0, 0]] + [other.at[:, 0] for other in others]
    pool = pool_ref.at[:, 0, 0]
    scatter_pages(slots, pieces, pool, bases)
    fresh = fresh_ref[:, 0, 0]
    patch(slots, length, pool, fresh)
    q = q_ref[0, 0]
    probs, new_prob = probabilities(
        q, [rows_of(piece[0]) for piece in pieces], bases, length, fresh[0]
    )
    out = mixed(probs, new_prob, [rows_of(piece[1]) for piece in pieces], fresh[1])
    out_ref[0, 0] = head_rows(out, head, jnp.zeros_like(out), heads).astype(out_ref.dtype)


def far_key_kernel(parts, slots, meta, *refs):
    pieces = refs[:parts]
    q_ref, fresh_ref, _, pool_ref, prob_ref, new_ref = refs[parts:]
    length, rank_part = meta[0], meta[2]
    pages = pieces[0].shape[1]
    bases = [(rank_part ^ e) * pages for e in range(parts)]
    pool = pool_ref.at[:, 0, 0]
    scatter_pages(slots, pieces, pool, bases)
    fresh = fresh_ref[:, 0, 0]
    patch(slots, length, pool, fresh)
    probs, new_prob = probabilities(
        q_ref[0, 0], [rows_of(piece[0]) for piece in pieces], bases, length, fresh[0]
    )
    for e, prob in enumerate(probs):
        prob_ref[e] = prob
    new_ref[...] = jnp.broadcast_to(new_prob, new_ref.shape)


def far_value_kernel(parts, heads, slots, meta, *refs):
    pieces = refs[:parts]
    prob_ref, new_ref, fresh_ref, kept_ref, _, pool_ref, out_ref = refs[parts:]
    length, head, rank_part = meta[0], meta[1], meta[2]
    pages = pieces[0].shape[1]
    bases = [(rank_part ^ e) * pages for e in range(parts)]
    pool = pool_ref.at[:, 0, 0]
    scatter_pages(slots, pieces, pool, bases)
    fresh = fresh_ref[:, 0, 0]
    patch(slots, length, pool, fresh)
    values = [rows_of(piece[0]) for piece in pieces]
    out = mixed([prob_ref[e] for e in range(parts)], new_ref[...], values, fresh[0])
    kept = kept_ref[0, 0].astype(jnp.float32)
    out_ref[0, 0] = head_rows(out, head, kept, heads).astype(out_ref.dtype)


def block_kernel(parts, heads, layer, slots, meta, *refs):
    pieces = refs[:parts]
    prob_ref, new_ref, fresh_ref, kept_ref = refs[parts : parts + 4]
    block_ref, sum_ref, token_ref, rest_ref = refs[2 * parts + 4 :]
    length, head, rank_part = meta[0], meta[1], meta[2]
    kind = fresh_ref.shape[0] - 1
    pages = prob_ref.shape[2] // PAGE
    bases = [(rank_part ^ e) * pages for e in range(parts)]
    scatter_pages(slots, pieces, block_ref, bases)
    fresh = fresh_ref[kind, layer, head]
    patch(slots, length, block_ref, fresh[None])
    values = [rows_of(piece[0]) for piece in pieces]
    out = mixed(
        [prob_ref[e, :, : values[e].shape[0]] for e in range(parts)],
        new_ref[...],
        values,
        fresh,
    )
    kept = kept_ref[layer, 0].astype(jnp.float32)
    sum_ref[...] = head_rows(out, head, kept, heads)
    token_ref[...] = fresh.astype(jnp.float32)
    rest_ref[...] = prob_ref[parts - 1, :, values[-1].shape[0] :]


def tail_kernel(
    parts, heads, layer, pages, slots, meta, piece, _block, sums, token, rest, _pool, _out,
    _piece, block, _sums, _token, _rest, pool, out, row_store, sems,
):
    length, head, rank_part = meta[0], meta[1], meta[2]
    kind = pool.shape[0] - 1
    tail_pages = piece.shape[1]
    slot_count = block.shape[1]
    base = (rank_part ^ (parts - 1)) * pages + pages - tail_pages
    scatter_pages(slots, [piece], block, [base])
    patch(slots, length, block, token[...][None])
    cuts = sems.shape[0] - 1
    size = slot_count // cuts
    stores = [
        pltpu.make_async_copy(
            block.at[0, pl.ds(i * size, size)],
            pool.at[kind, layer, head, pl.ds(i * size, size)],
            sems.at[i],
        )
        for i in range(cuts)
    ]
    for store in stores:
        store.start()
    share = lax.dot_general(
        rest[...], rows_of(piece[0]), (((1,), (0,)), ((), ())),
        preferred_element_type=jnp.float32,
    )
    done = sums[...]
    row_store[...] = head_rows(done + share, head, done, heads).astype(row_store.dtype)
    store = pltpu.make_async_copy(row_store, out.at[layer, 0], sems.at[cuts])
    store.start()
    store.wait()
    for store in stores:
        store.wait()


def cut_kernel(starts, src, *refs):
    outs, sems = refs[:-1], refs[-1]
    me = lax.axis_index("seq")
    copies = []
    for i, (distance, kind, layer, page) in enumerate(starts):
        kinds, layers, pages = outs[i].shape[0], outs[i].shape[1], outs[i].shape[2]
        for k in range(kinds):
            for l in range(layers):
                copies.append(
                    pltpu.make_async_copy(
                        src.at[kind + k, layer + l, me ^ distance, pl.ds(page, pages)],
                        outs[i].at[k, l],
                        sems.at[len(copies)],
                    )
                )
    for copy in copies:
        copy.start()
    for copy in copies:
        copy.wait()


def streamed(kv_prefill, queries, new_kv, lengths, page_slots):
    ranks = lax.axis_size("seq")
    me = lax.axis_index("seq")
    kinds, layers, seqs, block_rows, dim = kv_prefill.shape
    parts = CTX // block_rows
    heads = ranks // parts
    pages = block_rows // PAGE
    slot_count = page_slots.shape[1]
    q_rows = queries.shape[2]
    slots = page_slots[0]
    my_head, my_part = me // parts, me % parts
    first_head = lax.axis_index("tp") * heads
    fresh = lax.dynamic_slice_in_dim(new_kv, first_head, heads, 3)
    fresh = fresh.reshape(kinds, layers, heads, 1, dim)
    paged = kv_prefill.reshape(kinds, layers, seqs, pages, PAGE, dim)

    tail_pages = pages * TAIL // 128
    hbm_spec = pl.BlockSpec(memory_space=pl.ANY)
    vmem_spec = pl.BlockSpec(memory_space=pltpu.VMEM)
    smem_spec = pl.BlockSpec(memory_space=pltpu.SMEM)

    def cut(wanted, near_core):
        shapes = [entry[4:] + (PAGE, dim) for entry in wanted]
        return pl.pallas_call(
            functools.partial(cut_kernel, [entry[:4] for entry in wanted]),
            in_specs=[hbm_spec],
            out_specs=[vmem_spec if near_core else hbm_spec] * len(wanted),
            out_shape=[
                pltpu.VMEM(shape, kv_prefill.dtype)
                if near_core
                else jax.ShapeDtypeStruct(shape, kv_prefill.dtype)
                for shape in shapes
            ],
            scratch_shapes=[pltpu.SemaphoreType.DMA((sum(s[0] * s[1] for s in shapes),))],
            name="cut",
        )(paged)

    final = (kinds - 1, layers - 1, heads - 1)
    wanted = {}
    for kind in range(kinds):
        for layer in range(layers):
            for group in range(1, heads):
                for e in range(parts):
                    short = (kind, layer, group) == final and e == parts - 1
                    wanted["far", kind, layer, group, e] = (
                        group * parts + e, kind, layer, 0, 1, 1, pages - tail_pages * short,
                    )
                if (kind, layer, group) == (0, 0, 1):
                    for e in range(1, parts):
                        wanted["near", e] = (e, 0, 0, 0, kinds, layers, pages)
    wanted["tail"] = (
        ranks - 1, kinds - 1, layers - 1, pages - tail_pages, 1, 1, tail_pages,
    )
    entries = list(wanted.values())
    cuts = cut(entries[:1], True)
    cuts = list(cuts) + list(cut(entries[1:], False))
    received = {}
    for i, (key, entry) in enumerate(wanted.items()):
        pairs = [(r, r ^ entry[0]) for r in range(ranks)]
        received[key] = lax.ppermute(cuts[i], "seq", pairs)
    near = [received["near", e] for e in range(1, parts)]
    far = {
        key[1:4]: [received[("far",) + key[1:4] + (e,)][0] for e in range(parts)]
        for key in wanted
        if key[0] == "far"
    }
    tail = received["tail"][0]

    pool_shape = jax.ShapeDtypeStruct((kinds, layers, heads, slot_count, PAGE, dim), kv_prefill.dtype)
    out_shape = jax.ShapeDtypeStruct(queries.shape, queries.dtype)
    meta = jnp.stack([lengths[0], my_head, my_part, me]).astype(jnp.int32)
    pool, out = pl.pallas_call(
        functools.partial(own_kernel, parts, heads),
        grid_spec=pltpu.PrefetchScalarGridSpec(
            num_scalar_prefetch=2,
            grid=(layers,),
            in_specs=[
                pl.BlockSpec((kinds, 1, 1, pages, PAGE, dim), lambda l, s, m: (0, l, m[3], 0, 0, 0))
            ]
            + [
                pl.BlockSpec((kinds, 1, pages, PAGE, dim), lambda l, s, m: (0, l, 0, 0, 0))
                for _ in near
            ]
            + [
                pl.BlockSpec((1, 1, q_rows, dim), lambda l, s, m: (l, 0, 0, 0)),
                pl.BlockSpec((kinds, 1, 1, 1, dim), lambda l, s, m: (0, l, m[1], 0, 0)),
            ],
            out_specs=[
                pl.BlockSpec(
                    (kinds, 1, 1, slot_count, PAGE, dim), lambda l, s, m: (0, l, m[1], 0, 0, 0)
                ),
                pl.BlockSpec((1, 1, q_rows, dim), lambda l, s, m: (l, 0, 0, 0)),
            ],
        ),
        out_shape=(pool_shape, out_shape),
        name="own_head",
    )(slots, meta, paged, *near, queries, fresh)

    def piece_specs(pieces):
        return [pl.BlockSpec(piece.shape, lambda i, s, m: (0, 0, 0, 0)) for piece in pieces]

    weights = {}
    for kind in range(kinds):
        for layer in range(layers):
            for group in range(1, heads):
                meta = jnp.stack([lengths[0], my_head ^ group, my_part, me]).astype(jnp.int32)
                pieces = far[kind, layer, group]
                fresh_spec = pl.BlockSpec(
                    (1, 1, 1, 1, dim), lambda i, s, m, k=kind, l=layer: (k, l, m[1], 0, 0)
                )
                pool_spec = pl.BlockSpec(
                    (1, 1, 1, slot_count, PAGE, dim),
                    lambda i, s, m, k=kind, l=layer: (k, l, m[1], 0, 0, 0),
                )
                row_spec = pl.BlockSpec(
                    (1, 1, q_rows, dim), lambda i, s, m, l=layer: (l, 0, 0, 0)
                )
                prob_spec = pl.BlockSpec((parts, q_rows, block_rows), lambda i, s, m: (0, 0, 0))
                new_spec = pl.BlockSpec((q_rows, dim), lambda i, s, m: (0, 0))
                if kind == 0:
                    pool, *weights[layer, group] = pl.pallas_call(
                        functools.partial(far_key_kernel, parts),
                        grid_spec=pltpu.PrefetchScalarGridSpec(
                            num_scalar_prefetch=2,
                            grid=(1,),
                            in_specs=piece_specs(pieces) + [row_spec, fresh_spec, hbm_spec],
                            out_specs=[pool_spec, prob_spec, new_spec],
                        ),
                        out_shape=(
                            pool_shape,
                            jax.ShapeDtypeStruct((parts, q_rows, block_rows), jnp.bfloat16),
                            jax.ShapeDtypeStruct((q_rows, dim), jnp.float32),
                        ),
                        input_output_aliases={parts + 4: 0},
                        name="far_keys",
                    )(slots, meta, *pieces, queries, fresh, pool)
                elif (kind, layer, group) != final:
                    pool, out = pl.pallas_call(
                        functools.partial(far_value_kernel, parts, heads),
                        grid_spec=pltpu.PrefetchScalarGridSpec(
                            num_scalar_prefetch=2,
                            grid=(1,),
                            in_specs=piece_specs(pieces)
                            + [prob_spec, new_spec, fresh_spec, row_spec, hbm_spec],
                            out_specs=[pool_spec, row_spec],
                        ),
                        out_shape=(pool_shape, out_shape),
                        input_output_aliases={parts + 5: 1, parts + 6: 0},
                        name="far_values",
                    )(slots, meta, *pieces, *weights[layer, group], fresh, out, pool)
    block_shape = pltpu.VMEM((1, slot_count, PAGE, dim), kv_prefill.dtype)
    kept_shapes = [
        block_shape,
        pltpu.VMEM((q_rows, dim), jnp.float32),
        pltpu.VMEM((1, dim), jnp.float32),
        pltpu.VMEM((q_rows, tail_pages * PAGE), jnp.bfloat16),
    ]
    piece_shapes = [pltpu.VMEM(piece.shape, piece.dtype) for piece in pieces + [tail]]
    *_, block, mix, token, rest = pl.pallas_call(
        functools.partial(block_kernel, parts, heads, layers - 1),
        in_specs=[smem_spec] * 2 + [vmem_spec] * (parts + 4),
        out_specs=[vmem_spec] * (parts + 4),
        out_shape=piece_shapes[:-1]
        + kept_shapes,
        input_output_aliases={2 + e: e for e in range(parts)},
        name="last_block",
    )(slots, meta, *pieces, *weights[layers - 1, heads - 1], fresh, out)
    *_, pool, out = pl.pallas_call(
        functools.partial(tail_kernel, parts, heads, layers - 1, pages),
        in_specs=[smem_spec] * 2 + [vmem_spec] * 5 + [hbm_spec] * 2,
        out_specs=[vmem_spec] * 5 + [hbm_spec] * 2,
        out_shape=(piece_shapes[-1], *kept_shapes, pool_shape, out_shape),
        scratch_shapes=[
            pltpu.VMEM((q_rows, dim), queries.dtype),
            pltpu.SemaphoreType.DMA((5,)),
        ],
        input_output_aliases={2 + i: i for i in range(7)},
        name="tail_values",
    )(slots, meta, tail, block, mix, token, rest, pool, out)
    return pool, out


def body(kv_prefill, *rest):
    ranks = lax.axis_size("seq")
    block_rows = kv_prefill.shape[3]
    parts = CTX // block_rows
    if KVH % lax.axis_size("tp") == 0 and KVH // lax.axis_size("tp") * parts == ranks:
        return streamed(kv_prefill, *rest)
    return gathered(kv_prefill, *rest)


def solution(mesh):
    placed = (
        P(None, None, "groups", ("tp", "seq"), None),
        P(None, ("groups", "seq"), "tp", None),
        P(None, None, ("groups", "seq"), None, None),
        P(("groups", "seq")),
        P(("groups", "seq"), None),
    )
    return jax.shard_map(
        body,
        mesh=mesh,
        in_specs=placed,
        out_specs=(
            P(None, None, "tp", ("groups", "seq"), None, None),
            P(None, ("groups", "seq"), "tp", None),
        ),
        check_vma=False,
    )
```

```python
import functools
import math

import jax
import jax.numpy as jnp
from jax import lax
from jax.experimental import pallas as pl
from jax.experimental.pallas import tpu as pltpu
from jax.sharding import PartitionSpec as P


KVH = 8
PAGE = 16
CTX = 4096
TAIL = 32


def swapped(array, axis, bit):
    return lax.ppermute(array, axis, [(i, i ^ 1 << bit) for i in range(lax.axis_size(axis))])


def spread_heads(blocks, axis_dim):
    tp_ranks = lax.axis_size("tp")
    kv_rank = max(1, KVH // tp_ranks)
    fanout = tp_ranks * kv_rank // KVH
    levels = fanout.bit_length() - 1
    ordering = list(range(levels))
    my_rank = lax.axis_index("tp")
    finished = []
    for bit_index in ordering:
        partner = swapped(blocks, "tp", bit_index)
        lower_side = my_rank // (1 << bit_index) % 2 == 0
        lower_part = jnp.where(lower_side, blocks, partner)
        upper_part = jnp.where(lower_side, partner, blocks)
        higher_bits = sum((1 for earlier in finished if earlier > bit_index))
        shape_now = blocks.shape
        outer_count = 2**higher_bits
        split_shape = (
            shape_now[:axis_dim]
            + (outer_count, shape_now[axis_dim] // outer_count)
            + shape_now[axis_dim + 1 :]
        )
        paired = jnp.stack(
            (lower_part.reshape(split_shape), upper_part.reshape(split_shape)), axis=axis_dim + 1
        )
        blocks = paired.reshape(
            shape_now[:axis_dim] + (2 * shape_now[axis_dim],) + shape_now[axis_dim + 1 :]
        )
        finished.append(bit_index)
    return blocks


def repack(grouped, page_row, local_seqs):
    layers_here = grouped.shape[1]
    head_count = grouped.shape[3] // CTX
    head_dim = grouped.shape[4]
    paged_rows = grouped.reshape(
        2, layers_here, local_seqs, head_count, CTX // PAGE, PAGE, head_dim
    )
    paged_rows = paged_rows.transpose(0, 1, 3, 2, 4, 5, 6).reshape(
        2, layers_here, head_count, local_seqs * (CTX // PAGE), PAGE, head_dim
    )
    inverse = jnp.argsort(page_row)
    return jnp.take(paged_rows, inverse, axis=3)


def gathered(kv_prefill, queries, new_kv, lengths, page_slots):
    local_seqs = lengths.shape[0]
    page_row = page_slots[0]
    tp_ranks = lax.axis_size("tp")
    kv_rank = max(1, KVH // tp_ranks)
    layer_count = kv_prefill.shape[1]
    grouped = spread_heads(kv_prefill, 3)
    block_rows = kv_prefill.shape[3]
    fanout = grouped.shape[3] // block_rows
    shaped = grouped.reshape(
        2, layer_count, grouped.shape[2], fanout, 1, block_rows, grouped.shape[4]
    )
    pieces = lax.all_to_all(shaped, "seq", split_axis=2, concat_axis=4, tiled=True)
    flattened = pieces.reshape(
        2,
        pieces.shape[1],
        pieces.shape[2],
        pieces.shape[3] * pieces.shape[4] * pieces.shape[5],
        pieces.shape[6],
    )
    decode_pool = repack(flattened, page_row, local_seqs)
    first_head = lax.axis_index("tp") * KVH // tp_ranks
    fresh_rows = lax.dynamic_slice_in_dim(new_kv, first_head, kv_rank, 3)
    pages_per = CTX // PAGE
    length_now = lengths[0]
    slot_now = lax.dynamic_index_in_dim(page_row, 0 + length_now // PAGE, 0, False)
    update = fresh_rows[:, :, 0][:, :, :, None, None, :]
    decode_pool = lax.dynamic_update_slice(
        decode_pool, update, (0, 0, 0, slot_now, length_now % PAGE, 0)
    )
    slot_table = page_row.reshape(local_seqs, pages_per)
    head_dim = queries.shape[3]
    key_cache = jnp.take(decode_pool[0], slot_table, axis=2).reshape(
        layer_count, kv_rank, local_seqs, CTX, head_dim
    )
    values = jnp.take(decode_pool[1], slot_table, axis=2).reshape(
        layer_count, kv_rank, local_seqs, CTX, head_dim
    )
    grouped_q = queries.reshape(
        layer_count, local_seqs, kv_rank, queries.shape[2] // kv_rank, head_dim
    )
    scores = jnp.einsum(
        "lskgd,lkstd->lskgt", grouped_q, key_cache, preferred_element_type=jnp.float32
    ) * (1.0 / math.sqrt(head_dim))
    positions = jnp.arange(CTX, dtype=jnp.int32)
    visible = (positions[None, :] <= lengths[:, None])[None, :, None, None, :]
    masked = jnp.where(visible, scores, -1e30)
    highest = jnp.max(masked, axis=-1, keepdims=True)
    exponent = jnp.where(visible, jnp.exp(masked - highest), 0.0)
    weights = (exponent / jnp.sum(exponent, axis=-1, keepdims=True)).astype(jnp.bfloat16)
    mixed_out = jnp.einsum(
        "lskgt,lkstd->lskgd", weights, values, preferred_element_type=jnp.float32
    )
    attention_out = mixed_out.astype(jnp.bfloat16).reshape(queries.shape)
    return (decode_pool, attention_out)


def scatter_pages(slots, pieces, pool_ref, bases):
    for piece, base in zip(pieces, bases):
        kinds, pages = piece.shape[0], piece.shape[1]

        def move(j, carry):
            slot = slots[base + j]
            for k in range(kinds):
                pool_ref[k, slot] = piece[k, j]
            return carry

        lax.fori_loop(0, pages, move, 0, unroll=16)


def patch(slots, length, pool_ref, fresh):
    slot = slots[length // PAGE]
    for k in range(fresh.shape[0]):
        page = pool_ref[k, slot]
        row = lax.broadcasted_iota(jnp.int32, page.shape, 0)
        token = jnp.broadcast_to(fresh[k].astype(jnp.float32), page.shape)
        page = jnp.where(row == length % PAGE, token, page.astype(jnp.float32))
        pool_ref[k, slot] = page.astype(pool_ref.dtype)


def probabilities(q, keys, bases, length, fresh_key):
    scale = 1.0 / math.sqrt(q.shape[-1])
    new_score = jnp.sum(
        q.astype(jnp.float32) * fresh_key.astype(jnp.float32), axis=-1, keepdims=True
    ) * scale
    scores = []
    highest = new_score
    for key, base in zip(keys, bases):
        part = lax.dot_general(
            q, key, (((1,), (1,)), ((), ())), preferred_element_type=jnp.float32
        ) * scale
        position = base * PAGE + lax.broadcasted_iota(jnp.int32, part.shape, 1)
        part = jnp.where(position < length, part, -1e30)
        scores.append(part)
        highest = jnp.maximum(highest, jnp.max(part, axis=-1, keepdims=True))
    grown = [jnp.exp(part - highest) for part in scores]
    new_grown = jnp.exp(new_score - highest)
    total = new_grown
    for part in grown:
        total = total + jnp.sum(part, axis=-1, keepdims=True)
    inverse = 1.0 / total
    probs = [(part * inverse).astype(jnp.bfloat16) for part in grown]
    return probs, (new_grown * inverse).astype(jnp.bfloat16).astype(jnp.float32)


def mixed(probs, new_prob, values, fresh_value):
    out = new_prob * fresh_value.astype(jnp.float32)
    for prob, value in zip(probs, values):
        out = out + lax.dot_general(
            prob, value, (((1,), (0,)), ((), ())), preferred_element_type=jnp.float32
        )
    return out


def rows_of(piece):
    return piece.reshape(piece.shape[0] * piece.shape[1], piece.shape[2])


def head_rows(out, head, kept, heads):
    row = lax.broadcasted_iota(jnp.int32, out.shape, 0)
    mine = row // (out.shape[0] // heads) == head
    return jnp.where(mine, out, kept)


def own_kernel(parts, heads, slots, meta, own, *refs):
    others = refs[: parts - 1]
    q_ref, fresh_ref, pool_ref, out_ref = refs[parts - 1 :]
    length, head, rank_part = meta[0], meta[1], meta[2]
    pages = own.shape[3]
    bases = [(rank_part ^ e) * pages for e in range(parts)]
    pieces = [own.at[:, 0, 0]] + [other.at[:, 0] for other in others]
    pool = pool_ref.at[:, 0, 0]
    scatter_pages(slots, pieces, pool, bases)
    fresh = fresh_ref[:, 0, 0]
    patch(slots, length, pool, fresh)
    q = q_ref[0, 0]
    probs, new_prob = probabilities(
        q, [rows_of(piece[0]) for piece in pieces], bases, length, fresh[0]
    )
    out = mixed(probs, new_prob, [rows_of(piece[1]) for piece in pieces], fresh[1])
    out_ref[0, 0] = head_rows(out, head, jnp.zeros_like(out), heads).astype(out_ref.dtype)


def far_key_kernel(parts, slots, meta, *refs):
    pieces = refs[:parts]
    q_ref, fresh_ref, _, pool_ref, prob_ref, new_ref = refs[parts:]
    length, rank_part = meta[0], meta[2]
    pages = pieces[0].shape[1]
    bases = [(rank_part ^ e) * pages for e in range(parts)]
    pool = pool_ref.at[:, 0, 0]
    scatter_pages(slots, pieces, pool, bases)
    fresh = fresh_ref[:, 0, 0]
    patch(slots, length, pool, fresh)
    probs, new_prob = probabilities(
        q_ref[0, 0], [rows_of(piece[0]) for piece in pieces], bases, length, fresh[0]
    )
    for e, prob in enumerate(probs):
        prob_ref[e] = prob
    new_ref[...] = jnp.broadcast_to(new_prob, new_ref.shape)


def far_value_kernel(parts, heads, slots, meta, *refs):
    pieces = refs[:parts]
    prob_ref, new_ref, fresh_ref, kept_ref, _, pool_ref, out_ref = refs[parts:]
    length, head, rank_part = meta[0], meta[1], meta[2]
    pages = pieces[0].shape[1]
    bases = [(rank_part ^ e) * pages for e in range(parts)]
    pool = pool_ref.at[:, 0, 0]
    scatter_pages(slots, pieces, pool, bases)
    fresh = fresh_ref[:, 0, 0]
    patch(slots, length, pool, fresh)
    values = [rows_of(piece[0]) for piece in pieces]
    out = mixed([prob_ref[e] for e in range(parts)], new_ref[...], values, fresh[0])
    kept = kept_ref[0, 0].astype(jnp.float32)
    out_ref[0, 0] = head_rows(out, head, kept, heads).astype(out_ref.dtype)


def block_kernel(parts, heads, layer, slots, meta, *refs):
    pieces = refs[:parts]
    prob_ref, new_ref, fresh_ref, kept_ref = refs[parts : parts + 4]
    block_ref, sum_ref, token_ref, rest_ref = refs[2 * parts + 4 :]
    length, head, rank_part = meta[0], meta[1], meta[2]
    kind = fresh_ref.shape[0] - 1
    pages = prob_ref.shape[2] // PAGE
    bases = [(rank_part ^ e) * pages for e in range(parts)]
    scatter_pages(slots, pieces, block_ref, bases)
    fresh = fresh_ref[kind, layer, head]
    patch(slots, length, block_ref, fresh[None])
    values = [rows_of(piece[0]) for piece in pieces]
    out = mixed(
        [prob_ref[e, :, : values[e].shape[0]] for e in range(parts)],
        new_ref[...],
        values,
        fresh,
    )
    kept = kept_ref[layer, 0].astype(jnp.float32)
    sum_ref[...] = head_rows(out, head, kept, heads)
    token_ref[...] = fresh.astype(jnp.float32)
    rest_ref[...] = prob_ref[parts - 1, :, values[-1].shape[0] :]


def tail_kernel(
    parts, heads, layer, pages, slots, meta, piece, _block, sums, token, rest, _pool, _out,
    _piece, block, _sums, _token, _rest, pool, out, row_store, sems,
):
    length, head, rank_part = meta[0], meta[1], meta[2]
    kind = pool.shape[0] - 1
    tail_pages = piece.shape[1]
    slot_count = block.shape[1]
    base = (rank_part ^ (parts - 1)) * pages + pages - tail_pages
    scatter_pages(slots, [piece], block, [base])
    patch(slots, length, block, token[...][None])
    cuts = sems.shape[0] - 1
    size = slot_count // cuts
    stores = [
        pltpu.make_async_copy(
            block.at[0, pl.ds(i * size, size)],
            pool.at[kind, layer, head, pl.ds(i * size, size)],
            sems.at[i],
        )
        for i in range(cuts)
    ]
    for store in stores:
        store.start()
    share = lax.dot_general(
        rest[...], rows_of(piece[0]), (((1,), (0,)), ((), ())),
        preferred_element_type=jnp.float32,
    )
    done = sums[...]
    row_store[...] = head_rows(done + share, head, done, heads).astype(row_store.dtype)
    store = pltpu.make_async_copy(row_store, out.at[layer, 0], sems.at[cuts])
    store.start()
    store.wait()
    for store in stores:
        store.wait()


def cut_kernel(starts, bounced, src, *refs):
    outs, refs = refs[: len(starts)], refs[len(starts) :]
    load_sems, store_sems = refs[-2:]
    held = refs[:-2] if bounced else outs
    me = lax.axis_index("seq")
    loads, stores = [], []
    for i, (distance, kind, layer, page) in enumerate(starts):
        kinds, layers, pages = outs[i].shape[0], outs[i].shape[1], outs[i].shape[2]
        for k in range(kinds):
            for l in range(layers):
                loads.append(
                    pltpu.make_async_copy(
                        src.at[kind + k, layer + l, me ^ distance, pl.ds(page, pages)],
                        held[i].at[k, l],
                        load_sems.at[len(loads)],
                    )
                )
                if bounced:
                    stores.append(
                        pltpu.make_async_copy(
                            held[i].at[k, l], outs[i].at[k, l], store_sems.at[len(stores)]
                        )
                    )
    for load in loads:
        load.start()
    for i, load in enumerate(loads):
        load.wait()
        if bounced:
            stores[i].start()
    for store in stores:
        store.wait()


def streamed(kv_prefill, queries, new_kv, lengths, page_slots):
    ranks = lax.axis_size("seq")
    me = lax.axis_index("seq")
    kinds, layers, seqs, block_rows, dim = kv_prefill.shape
    parts = CTX // block_rows
    heads = ranks // parts
    pages = block_rows // PAGE
    slot_count = page_slots.shape[1]
    q_rows = queries.shape[2]
    slots = page_slots[0]
    my_head, my_part = me // parts, me % parts
    first_head = lax.axis_index("tp") * heads
    fresh = lax.dynamic_slice_in_dim(new_kv, first_head, heads, 3)
    fresh = fresh.reshape(kinds, layers, heads, 1, dim)
    paged = kv_prefill.reshape(kinds, layers, seqs, pages, PAGE, dim)

    tail_pages = pages * TAIL // 128
    hbm_spec = pl.BlockSpec(memory_space=pl.ANY)
    vmem_spec = pl.BlockSpec(memory_space=pltpu.VMEM)
    smem_spec = pl.BlockSpec(memory_space=pltpu.SMEM)

    def cut(wanted, near_core):
        shapes = [entry[4:] + (PAGE, dim) for entry in wanted]
        return pl.pallas_call(
            functools.partial(cut_kernel, [entry[:4] for entry in wanted], not near_core),
            in_specs=[hbm_spec],
            out_specs=[vmem_spec if near_core else hbm_spec] * len(wanted),
            out_shape=[
                pltpu.VMEM(shape, kv_prefill.dtype)
                if near_core
                else jax.ShapeDtypeStruct(shape, kv_prefill.dtype)
                for shape in shapes
            ],
            scratch_shapes=([] if near_core else [pltpu.VMEM(s, kv_prefill.dtype) for s in shapes])
            + [pltpu.SemaphoreType.DMA((sum(s[0] * s[1] for s in shapes),))] * 2,
            name="cut",
        )(paged)

    final = (kinds - 1, layers - 1, heads - 1)
    wanted = {}
    for kind in range(kinds):
        for layer in range(layers):
            for group in range(1, heads):
                for e in range(parts):
                    short = (kind, layer, group) == final and e == parts - 1
                    wanted["far", kind, layer, group, e] = (
                        group * parts + e, kind, layer, 0, 1, 1, pages - tail_pages * short,
                    )
                if (kind, layer, group) == (0, 0, 1):
                    for e in range(1, parts):
                        wanted["near", e] = (e, 0, 0, 0, kinds, layers, pages)
    wanted["tail"] = (
        ranks - 1, kinds - 1, layers - 1, pages - tail_pages, 1, 1, tail_pages,
    )
    entries = list(wanted.values())
    cuts = cut(entries[:1], True)
    cuts = list(cuts) + list(cut(entries[1:], False))
    received = {}
    for i, (key, entry) in enumerate(wanted.items()):
        pairs = [(r, r ^ entry[0]) for r in range(ranks)]
        received[key] = lax.ppermute(cuts[i], "seq", pairs)
    near = [received["near", e] for e in range(1, parts)]
    far = {
        key[1:4]: [received[("far",) + key[1:4] + (e,)][0] for e in range(parts)]
        for key in wanted
        if key[0] == "far"
    }
    tail = received["tail"][0]

    pool_shape = jax.ShapeDtypeStruct((kinds, layers, heads, slot_count, PAGE, dim), kv_prefill.dtype)
    out_shape = jax.ShapeDtypeStruct(queries.shape, queries.dtype)
    meta = jnp.stack([lengths[0], my_head, my_part, me]).astype(jnp.int32)
    pool, out = pl.pallas_call(
        functools.partial(own_kernel, parts, heads),
        grid_spec=pltpu.PrefetchScalarGridSpec(
            num_scalar_prefetch=2,
            grid=(layers,),
            in_specs=[
                pl.BlockSpec((kinds, 1, 1, pages, PAGE, dim), lambda l, s, m: (0, l, m[3], 0, 0, 0))
            ]
            + [
                pl.BlockSpec((kinds, 1, pages, PAGE, dim), lambda l, s, m: (0, l, 0, 0, 0))
                for _ in near
            ]
            + [
                pl.BlockSpec((1, 1, q_rows, dim), lambda l, s, m: (l, 0, 0, 0)),
                pl.BlockSpec((kinds, 1, 1, 1, dim), lambda l, s, m: (0, l, m[1], 0, 0)),
            ],
            out_specs=[
                pl.BlockSpec(
                    (kinds, 1, 1, slot_count, PAGE, dim), lambda l, s, m: (0, l, m[1], 0, 0, 0)
                ),
                pl.BlockSpec((1, 1, q_rows, dim), lambda l, s, m: (l, 0, 0, 0)),
            ],
        ),
        out_shape=(pool_shape, out_shape),
        name="own_head",
    )(slots, meta, paged, *near, queries, fresh)

    def piece_specs(pieces):
        return [pl.BlockSpec(piece.shape, lambda i, s, m: (0, 0, 0, 0)) for piece in pieces]

    weights = {}
    for kind in range(kinds):
        for layer in range(layers):
            for group in range(1, heads):
                meta = jnp.stack([lengths[0], my_head ^ group, my_part, me]).astype(jnp.int32)
                pieces = far[kind, layer, group]
                fresh_spec = pl.BlockSpec(
                    (1, 1, 1, 1, dim), lambda i, s, m, k=kind, l=layer: (k, l, m[1], 0, 0)
                )
                pool_spec = pl.BlockSpec(
                    (1, 1, 1, slot_count, PAGE, dim),
                    lambda i, s, m, k=kind, l=layer: (k, l, m[1], 0, 0, 0),
                )
                row_spec = pl.BlockSpec(
                    (1, 1, q_rows, dim), lambda i, s, m, l=layer: (l, 0, 0, 0)
                )
                prob_spec = pl.BlockSpec((parts, q_rows, block_rows), lambda i, s, m: (0, 0, 0))
                new_spec = pl.BlockSpec((q_rows, dim), lambda i, s, m: (0, 0))
                if kind == 0:
                    pool, *weights[layer, group] = pl.pallas_call(
                        functools.partial(far_key_kernel, parts),
                        grid_spec=pltpu.PrefetchScalarGridSpec(
                            num_scalar_prefetch=2,
                            grid=(1,),
                            in_specs=piece_specs(pieces) + [row_spec, fresh_spec, hbm_spec],
                            out_specs=[pool_spec, prob_spec, new_spec],
                        ),
                        out_shape=(
                            pool_shape,
                            jax.ShapeDtypeStruct((parts, q_rows, block_rows), jnp.bfloat16),
                            jax.ShapeDtypeStruct((q_rows, dim), jnp.float32),
                        ),
                        input_output_aliases={parts + 4: 0},
                        name="far_keys",
                    )(slots, meta, *pieces, queries, fresh, pool)
                elif (kind, layer, group) != final:
                    pool, out = pl.pallas_call(
                        functools.partial(far_value_kernel, parts, heads),
                        grid_spec=pltpu.PrefetchScalarGridSpec(
                            num_scalar_prefetch=2,
                            grid=(1,),
                            in_specs=piece_specs(pieces)
                            + [prob_spec, new_spec, fresh_spec, row_spec, hbm_spec],
                            out_specs=[pool_spec, row_spec],
                        ),
                        out_shape=(pool_shape, out_shape),
                        input_output_aliases={parts + 5: 1, parts + 6: 0},
                        name="far_values",
                    )(slots, meta, *pieces, *weights[layer, group], fresh, out, pool)
    block_shape = pltpu.VMEM((1, slot_count, PAGE, dim), kv_prefill.dtype)
    kept_shapes = [
        block_shape,
        pltpu.VMEM((q_rows, dim), jnp.float32),
        pltpu.VMEM((1, dim), jnp.float32),
        pltpu.VMEM((q_rows, tail_pages * PAGE), jnp.bfloat16),
    ]
    piece_shapes = [pltpu.VMEM(piece.shape, piece.dtype) for piece in pieces + [tail]]
    *_, block, mix, token, rest = pl.pallas_call(
        functools.partial(block_kernel, parts, heads, layers - 1),
        in_specs=[smem_spec] * 2 + [vmem_spec] * (parts + 4),
        out_specs=[vmem_spec] * (parts + 4),
        out_shape=piece_shapes[:-1]
        + kept_shapes,
        input_output_aliases={2 + e: e for e in range(parts)},
        name="last_block",
    )(slots, meta, *pieces, *weights[layers - 1, heads - 1], fresh, out)
    *_, pool, out = pl.pallas_call(
        functools.partial(tail_kernel, parts, heads, layers - 1, pages),
        in_specs=[smem_spec] * 2 + [vmem_spec] * 5 + [hbm_spec] * 2,
        out_specs=[vmem_spec] * 5 + [hbm_spec] * 2,
        out_shape=(piece_shapes[-1], *kept_shapes, pool_shape, out_shape),
        scratch_shapes=[
            pltpu.VMEM((q_rows, dim), queries.dtype),
            pltpu.SemaphoreType.DMA((5,)),
        ],
        input_output_aliases={2 + i: i for i in range(7)},
        name="tail_values",
    )(slots, meta, tail, block, mix, token, rest, pool, out)
    return pool, out


def body(kv_prefill, *rest):
    ranks = lax.axis_size("seq")
    block_rows = kv_prefill.shape[3]
    parts = CTX // block_rows
    if KVH % lax.axis_size("tp") == 0 and KVH // lax.axis_size("tp") * parts == ranks:
        return streamed(kv_prefill, *rest)
    return gathered(kv_prefill, *rest)


def solution(mesh):
    placed = (
        P(None, None, "groups", ("tp", "seq"), None),
        P(None, ("groups", "seq"), "tp", None),
        P(None, None, ("groups", "seq"), None, None),
        P(("groups", "seq")),
        P(("groups", "seq"), None),
    )
    return jax.shard_map(
        body,
        mesh=mesh,
        in_specs=placed,
        out_specs=(
            P(None, None, "tp", ("groups", "seq"), None, None),
            P(None, ("groups", "seq"), "tp", None),
        ),
        check_vma=False,
    )
```
